32 devices in a mesh: rep: 1 (over z), emb: 4 (over y), model: 8 (over x, core).
Axes of the slice: x: 4, y: 4, z: 1, core: 2. Of those that a mesh axis runs over, the one named last changes fastest.
The devices are a block of a 4x4x8 slice.
Arguments:
- x: bfloat16 [512, 4096], P('rep')
- Wq: bfloat16 [4096, 4096], P('emb', 'model')
- Wk: bfloat16 [4096, 256], replicated
- Wv: bfloat16 [4096, 256], replicated
- Wo: bfloat16 [4096, 4096], P('model', 'emb')
- Kc: bfloat16 [512, 512, 256], P('rep')
- Vc: bfloat16 [512, 512, 256], P('rep')
- lengths: int32 [512], P('rep')
Outputs:
- output 1: bfloat16 [512, 4096], P('rep')
- output 2: bfloat16 [512, 256], P('rep')
- output 3: bfloat16 [512, 256], P('rep')
All inputs are finite; a program needn't handle non-finite values.
Results may differ from the reference program's by a relative error of at most 0.0128483.
Values are sent between devices in bfloat16 or wider.
A program may use at most 768 MiB of HBM per device.

```python
import jax
import jax.numpy as jnp
from jax import lax

B = 512
T = 512
D = 4096
H = 16
DH = 256


def setup_inputs(seed: int = 0, part: int = 0) -> dict:
    kshared, kpart = jax.random.split(jax.random.key(seed))
    kpart = jax.random.fold_in(kpart, part)
    kq, kk, kv, ko = jax.random.split(kshared, 4)
    kx, kkc, kvc, kl = jax.random.split(kpart, 4)
    x = jax.random.normal(kx, (B, D), jnp.float32)
    Wq = jax.random.normal(kq, (D, H * DH), jnp.float32) * (2.5 * D ** -0.5)
    Wk = jax.random.normal(kk, (D, DH), jnp.float32) * D ** -0.5
    Wv = jax.random.normal(kv, (D, DH), jnp.float32) * D ** -0.5
    Wo = jax.random.normal(ko, (H * DH, D), jnp.float32) * (3.0 * (H * DH) ** -0.5)
    Kc = jax.random.normal(kkc, (B, T, DH), jnp.float32)
    Vc = jax.random.normal(kvc, (B, T, DH), jnp.float32)
    kl1, kl2, kl3 = jax.random.split(jax.random.fold_in(kl, 7), 3)
    full = T - 1 - jax.random.randint(kl1, (B,), 0, T // 8)
    tiny = jax.random.randint(kl2, (B,), 1, 9)
    lengths = jnp.where(jax.random.bernoulli(kl3, 0.5, (B,)), full, tiny).astype(jnp.int32)
    bf = jnp.bfloat16
    return {'x': x.astype(bf), 'Wq': Wq.astype(bf), 'Wk': Wk.astype(bf), 'Wv': Wv.astype(bf),
            'Wo': Wo.astype(bf), 'Kc': Kc.astype(bf), 'Vc': Vc.astype(bf), 'lengths': lengths}


def reference(x, Wq, Wk, Wv, Wo, Kc, Vc, lengths):
    scale = DH ** -0.5
    q = jnp.dot(x, Wq, preferred_element_type=jnp.float32).astype(jnp.bfloat16).reshape(B, H, DH)
    k_new = jnp.dot(x, Wk, preferred_element_type=jnp.float32).astype(jnp.bfloat16)
    v_new = jnp.dot(x, Wv, preferred_element_type=jnp.float32).astype(jnp.bfloat16)
    pos = jnp.arange(T)

    def one(a):
        qb, Kb, Vb, kn, vn, n = a
        s = jnp.dot(qb, Kb.T, preferred_element_type=jnp.float32) * scale
        s = jnp.where(pos[None, :] < n, s, -jnp.inf)
        sn = jnp.dot(qb, kn, preferred_element_type=jnp.float32) * scale
        m = jnp.maximum(jnp.max(s, axis=1), sn)
        p = jnp.exp(s - m[:, None])
        pn = jnp.exp(sn - m)
        l = jnp.sum(p, axis=1) + pn
        acc = jnp.dot(p.astype(jnp.bfloat16), Vb, preferred_element_type=jnp.float32)
        acc = acc + pn.astype(jnp.bfloat16).astype(jnp.float32)[:, None] * vn.astype(jnp.float32)[None, :]
        return (acc / l[:, None]).astype(jnp.bfloat16)

    o = lax.map(one, (q, Kc, Vc, k_new, v_new, lengths))
    y = x.astype(jnp.float32) + jnp.dot(o.reshape(B, H * DH), Wo, preferred_element_type=jnp.float32)
    return y.astype(jnp.bfloat16), k_new, v_new
```

```python
import functools

import jax
import jax.numpy as jnp
from jax import lax
from jax.experimental import pallas as pl
from jax.experimental.pallas import tpu as pltpu
from jax.sharding import PartitionSpec as P

CORES = 2
LANES = 128
F32 = jnp.float32
BF16 = jnp.bfloat16


def _mod(a, n):
    return lax.rem(a + 2 * n, n)


def _kernel(ne, nm, H, lens_ref, x_hbm, wq_hbm, wk_hbm, wv_hbm, wo_hbm, kc_hbm, vc_hbm,
            y_ref, kn_ref, vn_ref,
            xv, wq_v, wkv, k_v, v_v, wo_v, s_opp, s_up, s_dn, s_own, rel_p, rel_m, fin_p, fin_m,
            qb, qr, q32, kv32, o32, o_all,
            lsem, q_ss, q_rs, a_ss, a_rs, w_ss, w_rs, d_ss, d_rs, o_ss, o_rs, y_ss, y_rs, c_ss, c_rs):
    nx = nm // CORES
    i = lax.axis_index('emb')
    j = lax.axis_index('model')
    X = lax.div(j, CORES)
    c = lax.rem(j, CORES)
    de = xv.shape[2]
    be = s_opp.shape[0]
    bl = qr.shape[1]
    nl = q32.shape[0]
    dh = nl * LANES
    hl = H // nm
    nw = wo_v.shape[2]
    hb = be // 2
    start = pl.multiple_of(i * be + j * bl, bl)
    T = k_v.shape[1]
    scale = dh ** -0.5

    def dev(yy, xx, cc):
        return {'emb': yy, 'model': xx * CORES + cc}

    def row(jj):
        return {'emb': i, 'model': jj}

    def rcopy(src, dst, ss, rs, to):
        return pltpu.make_async_remote_copy(src_ref=src, dst_ref=dst, send_sem=ss, recv_sem=rs,
                                            device_id=to, device_id_type=pl.DeviceIdType.MESH)

    up, dn, opp = _mod(i + 1, ne), _mod(i - 1, ne), _mod(i + 2, ne)
    partner = dev(i, X, 1 - c)

    barrier = pltpu.get_barrier_semaphore()
    for k in range(1, nm):
        pl.semaphore_signal(barrier, inc=1, device_id=row(_mod(j + k, nm)), device_id_type=pl.DeviceIdType.MESH)
    for yy in (up, dn):
        pl.semaphore_signal(barrier, inc=1, device_id={'emb': yy, 'model': j}, device_id_type=pl.DeviceIdType.MESH)

    def load(n, src, dst):
        cp = pltpu.make_async_copy(src, dst, lsem.at[n])
        cp.start()
        return cp

    def xblock(n, blk):
        return load(n, x_hbm.at[:, pl.ds(pl.multiple_of(blk * de, de), de)], xv.at[blk])

    ld_x = [xblock(0, i)]
    ld_wq = load(4, wq_hbm, wq_v)
    ld_x += [xblock(k, _mod(i + k, ne)) for k in range(1, ne)]
    ld_wk = load(5, wk_hbm, wkv.at[:, pl.ds(0, dh)])
    ld_wv = load(6, wv_hbm, wkv.at[:, pl.ds(dh, dh)])
    ld_k = load(7, kc_hbm.at[pl.ds(start, bl)], k_v)
    ld_v = load(8, vc_hbm.at[pl.ds(start, bl)], v_v)
    ld_wo = load(9, wo_hbm.at[:, pl.ds(pl.multiple_of(X * nw, nw), nw)], wo_v.at[j])

    pl.semaphore_wait(barrier, nm - 1 + 2)

    sends = []

    def go(cp):
        cp.start()
        sends.append(cp)

    for k in (1, nx - 1, *range(2, nx - 1)):
        t = _mod(X + k, nx)
        go(rcopy(wo_hbm.at[:, pl.ds(pl.multiple_of(t * nw, nw), nw)], wo_v.at[j], w_ss.at[k], w_rs.at[k],
                 dev(i, t, c)))

    ld_x[0].wait()
    ld_wq.wait()

    def part(d, buf):
        buf[...] = jnp.dot(xv[i, pl.ds(pl.multiple_of(d * be, be), be), :], wq_v[...], preferred_element_type=F32)

    lo, hi = pl.ds(0, hb), pl.ds(hb, hb)
    to_up, to_dn = {'emb': up, 'model': j}, {'emb': dn, 'model': j}
    part(opp, s_opp)
    go(rcopy(s_opp.at[lo], rel_p, q_ss.at[0], q_rs.at[0], to_up))
    go(rcopy(s_opp.at[hi], rel_m, q_ss.at[1], q_rs.at[1], to_dn))
    part(up, s_up)
    go(rcopy(s_up.at[hi], fin_p.at[hi], q_ss.at[2], q_rs.at[2], to_up))
    part(dn, s_dn)
    go(rcopy(s_dn.at[lo], fin_m.at[lo], q_ss.at[3], q_rs.at[3], to_dn))
    part(i, s_own)

    for ld in ld_x[1:]:
        ld.wait()
    ld_wk.wait()
    ld_wv.wait()

    rows_m = kn_ref.shape[0] // ne

    def kv_rows(m, _):
        rows = pl.ds(pl.multiple_of(m * rows_m, rows_m), rows_m)
        acc = jnp.dot(xv[0, rows, :], wkv[0:de, :], preferred_element_type=F32)
        for blk in range(1, ne):
            acc = acc + jnp.dot(xv[blk, rows, :], wkv[blk * de:(blk + 1) * de, :], preferred_element_type=F32)
        kn_ref[rows, :] = acc[:, :dh].astype(BF16)
        vn_ref[rows, :] = acc[:, dh:].astype(BF16)
        return 0

    lax.fori_loop(0, ne, kv_rows, 0)

    rcopy(rel_p, rel_p, q_ss.at[0], q_rs.at[0], to_up).wait_recv()
    s_up[0:hb, :] = s_up[0:hb, :] + rel_p[...]
    go(rcopy(s_up.at[lo], fin_p.at[lo], q_ss.at[4], q_rs.at[4], to_up))
    rcopy(rel_m, rel_m, q_ss.at[1], q_rs.at[1], to_dn).wait_recv()
    s_dn[hb:be, :] = s_dn[hb:be, :] + rel_m[...]
    go(rcopy(s_dn.at[hi], fin_m.at[hi], q_ss.at[5], q_rs.at[5], to_dn))

    rcopy(fin_p.at[hi], fin_p.at[hi], q_ss.at[2], q_rs.at[2], to_up).wait_recv()
    rcopy(fin_m.at[lo], fin_m.at[lo], q_ss.at[3], q_rs.at[3], to_dn).wait_recv()
    rcopy(fin_p.at[lo], fin_p.at[lo], q_ss.at[4], q_rs.at[4], to_up).wait_recv()
    rcopy(fin_m.at[hi], fin_m.at[hi], q_ss.at[5], q_rs.at[5], to_dn).wait_recv()
    qb[...] = (s_own[...] + fin_p[...] + fin_m[...]).astype(BF16).reshape(qb.shape)
    for k in range(1, nm):
        t = _mod(j + k, nm)
        go(rcopy(qb.at[t], qr.at[j], a_ss.at[k], a_rs.at[k], row(t)))
    qr[j] = qb[j]

    ld_wo.wait()
    go(rcopy(wo_v.at[j], wo_v.at[j], d_ss.at[0], d_rs.at[0], partner))
    for k in range(1, nx):
        src = _mod(X - k, nx) * CORES + c
        rcopy(wo_v.at[src], wo_v.at[src], w_ss.at[k], w_rs.at[k], partner).wait_recv()
        go(rcopy(wo_v.at[src], wo_v.at[src], d_ss.at[k], d_rs.at[k], partner))

    kv32[0] = kn_ref[pl.ds(start, bl), :].astype(F32)
    kv32[1] = vn_ref[pl.ds(start, bl), :].astype(F32)
    ld_k.wait()
    ld_v.wait()

    for k in range(1, nm):
        src = _mod(j - k, nm)
        rcopy(qr.at[src], qr.at[src], a_ss.at[k], a_rs.at[k], partner).wait_recv()
    for jj in range(nm):
        for h in range(hl):
            for n in range(nl):
                q32[n, (jj * hl + h) * bl:(jj * hl + h + 1) * bl, :] = (
                    qr[jj, :, h * dh + n * LANES:h * dh + (n + 1) * LANES].astype(F32))

    def attend(b, _):
        q = jnp.concatenate([q32[n, pl.ds(b, H, stride=bl), :] for n in range(nl)], axis=1)
        s = lax.dot_general(q.astype(BF16), k_v[b], (((1,), (1,)), ((), ())), preferred_element_type=F32) * scale
        n = lens_ref[start + b]
        s = jnp.where(lax.broadcasted_iota(jnp.int32, (H, T), 1) < n, s, -jnp.inf)
        sn = jnp.sum(q * kv32[0, pl.ds(b, 1), :], axis=1, keepdims=True) * scale
        m = jnp.maximum(jnp.max(s, axis=1, keepdims=True), sn)
        p = jnp.exp(s - m)
        pn = jnp.exp(sn - m)
        l = jnp.sum(p, axis=1, keepdims=True) + pn
        acc = jnp.dot(p.astype(BF16), v_v[b], preferred_element_type=F32)
        acc = acc + pn.astype(BF16).astype(F32) * kv32[1, pl.ds(b, 1), :]
        o = acc / l
        for n in range(nl):
            o32[n, pl.ds(b, H, stride=bl), :] = o[:, n * LANES:(n + 1) * LANES]
        return 0

    lax.fori_loop(0, bl, attend, 0, unroll=4)

    chip = i * nx + X
    for h in range(H):
        for n in range(nl):
            o_all[h, chip, :, n * LANES:(n + 1) * LANES] = o32[n, h * bl:(h + 1) * bl, :].astype(BF16)

    def gather(piece, ss, rs, arrived):
        class Half:
            def __init__(self, n):
                self.base, self.q = n * 20, 2 * n
                self.x_first = n == 0

            def piece(self, dp, ds, q, n):
                if self.x_first:
                    return piece(_mod(i + ds, ne), _mod(X + dp, nx), self.q + q, n)
                return piece(_mod(i + dp, ne), _mod(X + ds, nx), self.q + q, n)

            def to(self, dp, ds):
                if self.x_first:
                    return dev(_mod(i + ds, ne), _mod(X + dp, nx), c)
                return dev(_mod(i + dp, ne), _mod(X + ds, nx), c)

            def send(self, mid, ref, to):
                go(rcopy(ref, ref, ss.at[self.base + mid], rs.at[self.base + mid], to))

            def wait(self, mid, ref):
                rcopy(ref, ref, ss.at[self.base + mid], rs.at[self.base + mid], partner).wait_recv()
                arrived(ref)

            def s1(self):
                for d, sg in enumerate((1, -1)):
                    self.send(d, self.piece(0, 0, 0, 2), self.to(sg, 0))

            def w1s2(self):
                for d, sg in enumerate((1, -1)):
                    self.wait(d, self.piece(-sg, 0, 0, 2))
                    self.send(2 + d, self.piece(-sg, 0, d, 1), self.to(sg, 0))

            def w2(self):
                for d, sg in enumerate((1, -1)):
                    self.wait(2 + d, self.piece(2, 0, d, 1))

            def s3(self, k):
                for d, sg in enumerate((1, -1)):
                    self.send(4 + 2 * k + d, self.piece(ITEMS[k], 0, 0, 2), self.to(0, sg))

            def w3s4(self, k):
                for d, sg in enumerate((1, -1)):
                    self.wait(4 + 2 * k + d, self.piece(ITEMS[k], -sg, 0, 2))
                    self.send(12 + 2 * k + d, self.piece(ITEMS[k], -sg, d, 1), self.to(0, sg))

            def w4(self, k):
                for d, sg in enumerate((1, -1)):
                    self.wait(12 + 2 * k + d, self.piece(ITEMS[k], 2, d, 1))

        ITEMS = (0, -1, 1, 2)
        halves = (Half(0), Half(1))

        def both(name, *a):
            for hf in halves:
                getattr(hf, name)(*a)

        both('s1')
        both('s3', 0)
        arrived(piece(i, X, 0, 4))
        both('w1s2')
        both('s3', 1)
        both('s3', 2)
        both('w3s4', 0)
        both('w2')
        both('s3', 3)
        both('w3s4', 1)
        both('w3s4', 2)
        both('w3s4', 3)
        for k in range(4):
            both('w4', k)

    hq = H // 4
    gather(lambda yy, xx, q, n: o_all.at[pl.ds(q * hq, n * hq), yy * nx + xx], o_ss, o_rs, lambda ref: None)

    for k in range(nx):
        src = _mod(X - k, nx) * CORES + (1 - c)
        rcopy(wo_v.at[src], wo_v.at[src], d_ss.at[k], d_rs.at[k], partner).wait_recv()

    rows = ne * nx * bl
    acc = None
    for h in range(H):
        t = jnp.dot(o_all[h].reshape(rows, dh), wo_v[h // hl, (h % hl) * dh:(h % hl + 1) * dh, :],
                    preferred_element_type=F32)
        acc = t if acc is None else acc + t
    cols = pl.ds(pl.multiple_of(chip * nw, nw), nw)
    mine = pl.ds(pl.multiple_of(X * nw, nw), nw)
    for r in range(ne):
        for xx in range(nx):
            g = (r * nx + xx) * bl
            res = xv[i, pl.ds(pl.multiple_of(r * be + (xx * CORES + c) * bl, bl), bl), mine].astype(F32)
            y_ref[r, xx, c, :, cols] = (res + acc[g:g + bl, :].astype(BF16).astype(F32)).astype(BF16)

    def to_partner(ref):
        rcopy(ref, ref, c_ss, c_rs, partner).start()

    gather(lambda yy, xx, q, n: y_ref.at[pl.ds(q, n), :, c, :, pl.ds(pl.multiple_of((yy * nx + xx) * nw, nw), nw)],
           y_ss, y_rs, to_partner)

    other, own = y_ref.at[:, :, 1 - c], y_ref.at[:, :, c]
    rcopy(own, other, c_ss, c_rs, partner).wait_recv()
    rcopy(own, other, c_ss, c_rs, partner).wait_send()
    for cp in sends:
        cp.wait_send()


def solution(mesh):
    ne = mesh.shape['emb']
    nm = mesh.shape['model']

    def local(x, Wq, Wk, Wv, Wo, Kc, Vc, lengths):
        b, d = x.shape
        de = Wq.shape[0]
        dh = Wk.shape[1]
        hl = Wq.shape[1] // dh
        H = hl * nm
        nx = nm // CORES
        be = b // ne
        bl = be // nm
        T = Kc.shape[1]
        nw = Wo.shape[1] // nx
        hd = hl * dh
        V = pltpu.VMEM
        DMA = pltpu.SemaphoreType.DMA
        hbm = pl.BlockSpec(memory_space=pl.ANY)
        vmem = pl.BlockSpec(memory_space=pltpu.VMEM)
        y, kn, vn = pl.pallas_call(
            functools.partial(_kernel, ne, nm, H),
            out_shape=(jax.ShapeDtypeStruct((ne, nx, CORES, bl, d), BF16),
                       jax.ShapeDtypeStruct((b, dh), BF16),
                       jax.ShapeDtypeStruct((b, dh), BF16)),
            in_specs=[pl.BlockSpec(memory_space=pltpu.SMEM)] + [hbm] * 7,
            out_specs=(vmem, vmem, vmem),
            scratch_shapes=[
                V((ne, b, de), BF16), V((de, hd), BF16), V((d, 2 * dh), BF16),
                V((bl, T, dh), BF16), V((bl, T, dh), BF16), V((nm, hd, nw), BF16),
                V((be, hd), F32), V((be, hd), F32), V((be, hd), F32), V((be, hd), F32),
                V((be // 2, hd), F32), V((be // 2, hd), F32), V((be, hd), F32), V((be, hd), F32),
                V((nm, bl, hd), BF16), V((nm, bl, hd), BF16), V((dh // LANES, H * bl, LANES), F32),
                V((2, bl, dh), F32), V((dh // LANES, H * bl, LANES), F32), V((H, ne * nx, bl, dh), BF16),
                DMA((10,)), DMA((6,)), DMA((6,)), DMA((nm,)), DMA((nm,)), DMA((nx,)), DMA((nx,)),
                DMA((nx,)), DMA((nx,)), DMA((40,)), DMA((40,)), DMA((40,)), DMA((40,)), DMA, DMA,
            ],
            compiler_params=pltpu.CompilerParams(collective_id=0, has_side_effects=True,
                                                 vmem_limit_bytes=60 * 1024 * 1024),
        )(lengths, x, Wq, Wk, Wv, Wo, Kc, Vc)
        return y.reshape(b, d), kn, vn

    in_specs = (P('rep', None), P('emb', 'model'), P(), P(), P('model', 'emb'),
                P('rep', None, None), P('rep', None, None), P('rep'))
    out_specs = (P('rep', None), P('rep', None), P('rep', None))
    return jax.shard_map(local, mesh=mesh, in_specs=in_specs, out_specs=out_specs, check_vma=False)
```

```python
import functools

import jax
import jax.numpy as jnp
from jax import lax
from jax.experimental import pallas as pl
from jax.experimental.pallas import tpu as pltpu
from jax.sharding import PartitionSpec as P

CORES = 2
LANES = 128
F32 = jnp.float32
BF16 = jnp.bfloat16


def _mod(a, n):
    return lax.rem(a + 2 * n, n)


def _kernel(ne, nm, H, lens_ref, x_hbm, wq_hbm, wk_hbm, wv_hbm, wo_hbm, kc_hbm, vc_hbm,
            y_ref, kn_ref, vn_ref,
            xv, wq_v, wkv, k_v, v_v, wo_v, s_opp, s_up, s_dn, s_own, rel_p, rel_m, fin_p, fin_m,
            wo_rel, qb, qr, q32, kv32, o32, o_all,
            lsem, q_ss, q_rs, a_ss, a_rs, w_ss, w_rs, d_ss, d_rs, o_ss, o_rs, y_ss, y_rs, c_ss, c_rs):
    nx = nm // CORES
    i = lax.axis_index('emb')
    j = lax.axis_index('model')
    X = lax.div(j, CORES)
    c = lax.rem(j, CORES)
    de = xv.shape[2]
    be = s_opp.shape[0]
    bl = qr.shape[1]
    nl = q32.shape[0]
    dh = nl * LANES
    hl = H // nm
    hd, nw = wo_v.shape[1:]
    hb = be // 2
    start = pl.multiple_of(i * be + j * bl, bl)
    T = k_v.shape[1]
    scale = dh ** -0.5

    def dev(yy, xx, cc):
        return {'emb': yy, 'model': xx * CORES + cc}

    def row(jj):
        return {'emb': i, 'model': jj}

    def rcopy(src, dst, ss, rs, to):
        return pltpu.make_async_remote_copy(src_ref=src, dst_ref=dst, send_sem=ss, recv_sem=rs,
                                            device_id=to, device_id_type=pl.DeviceIdType.MESH)

    up, dn, opp = _mod(i + 1, ne), _mod(i - 1, ne), _mod(i + 2, ne)
    partner = dev(i, X, 1 - c)

    barrier = pltpu.get_barrier_semaphore()
    for k in range(1, nm):
        pl.semaphore_signal(barrier, inc=1, device_id=row(_mod(j + k, nm)), device_id_type=pl.DeviceIdType.MESH)
    for yy in (up, dn):
        pl.semaphore_signal(barrier, inc=1, device_id={'emb': yy, 'model': j}, device_id_type=pl.DeviceIdType.MESH)

    def load(n, src, dst):
        cp = pltpu.make_async_copy(src, dst, lsem.at[n])
        cp.start()
        return cp

    def xblock(n, blk):
        return load(n, x_hbm.at[:, pl.ds(pl.multiple_of(blk * de, de), de)], xv.at[blk])

    ld_x = [xblock(0, i)]
    ld_wq = load(4, wq_hbm, wq_v)
    ld_x += [xblock(k, _mod(i + k, ne)) for k in range(1, ne)]
    ld_wk = load(5, wk_hbm, wkv.at[:, pl.ds(0, dh)])
    ld_wv = load(6, wv_hbm, wkv.at[:, pl.ds(dh, dh)])
    ld_k = load(7, kc_hbm.at[pl.ds(start, bl)], k_v)
    ld_v = load(8, vc_hbm.at[pl.ds(start, bl)], v_v)
    ld_wo = load(9, wo_hbm.at[:, pl.ds(pl.multiple_of(X * nw, nw), nw)], wo_v.at[j])

    sends = []

    def go(cp):
        cp.start()
        sends.append(cp)

    ld_x[0].wait()
    ld_wq.wait()

    def part(d, buf):
        buf[...] = jnp.dot(xv[i, pl.ds(pl.multiple_of(d * be, be), be), :], wq_v[...], preferred_element_type=F32)

    lo, hi = pl.ds(0, hb), pl.ds(hb, hb)
    to_up, to_dn = {'emb': up, 'model': j}, {'emb': dn, 'model': j}
    part(opp, s_opp)
    pl.semaphore_wait(barrier, nm - 1 + 2)
    go(rcopy(s_opp.at[lo], rel_p, q_ss.at[0], q_rs.at[0], to_up))
    go(rcopy(s_opp.at[hi], rel_m, q_ss.at[1], q_rs.at[1], to_dn))
    east, west, far = _mod(X + 1, nx), _mod(X - 1, nx), _mod(X + 2, nx)
    wo_lo, wo_hi = pl.ds(0, hd // 2), pl.ds(hd // 2, hd // 2)

    def wo_cols(rows, t):
        return wo_hbm.at[rows, pl.ds(pl.multiple_of(t * nw, nw), nw)]

    go(rcopy(wo_cols(pl.ds(0, hd), east), wo_v.at[j], w_ss.at[0], w_rs.at[0], dev(i, east, c)))
    go(rcopy(wo_cols(pl.ds(0, hd), west), wo_v.at[j], w_ss.at[1], w_rs.at[1], dev(i, west, c)))
    go(rcopy(wo_cols(wo_lo, far), wo_rel.at[0], w_ss.at[2], w_rs.at[2], dev(i, east, c)))
    go(rcopy(wo_cols(wo_hi, far), wo_rel.at[1], w_ss.at[3], w_rs.at[3], dev(i, west, c)))

    part(up, s_up)
    go(rcopy(s_up.at[hi], fin_p.at[hi], q_ss.at[2], q_rs.at[2], to_up))
    part(dn, s_dn)
    go(rcopy(s_dn.at[lo], fin_m.at[lo], q_ss.at[3], q_rs.at[3], to_dn))
    part(i, s_own)

    for ld in ld_x[1:]:
        ld.wait()
    ld_wk.wait()
    ld_wv.wait()

    rows_m = kn_ref.shape[0] // ne

    def kv_rows(m, _):
        rows = pl.ds(pl.multiple_of(m * rows_m, rows_m), rows_m)
        acc = jnp.dot(xv[0, rows, :], wkv[0:de, :], preferred_element_type=F32)
        for blk in range(1, ne):
            acc = acc + jnp.dot(xv[blk, rows, :], wkv[blk * de:(blk + 1) * de, :], preferred_element_type=F32)
        kn_ref[rows, :] = acc[:, :dh].astype(BF16)
        vn_ref[rows, :] = acc[:, dh:].astype(BF16)
        return 0

    lax.fori_loop(0, ne, kv_rows, 0)

    rcopy(rel_p, rel_p, q_ss.at[0], q_rs.at[0], to_up).wait_recv()
    s_up[0:hb, :] = s_up[0:hb, :] + rel_p[...]
    go(rcopy(s_up.at[lo], fin_p.at[lo], q_ss.at[4], q_rs.at[4], to_up))
    rcopy(rel_m, rel_m, q_ss.at[1], q_rs.at[1], to_dn).wait_recv()
    s_dn[hb:be, :] = s_dn[hb:be, :] + rel_m[...]
    go(rcopy(s_dn.at[hi], fin_m.at[hi], q_ss.at[5], q_rs.at[5], to_dn))

    rcopy(fin_p.at[hi], fin_p.at[hi], q_ss.at[2], q_rs.at[2], to_up).wait_recv()
    rcopy(fin_m.at[lo], fin_m.at[lo], q_ss.at[3], q_rs.at[3], to_dn).wait_recv()
    rcopy(fin_p.at[lo], fin_p.at[lo], q_ss.at[4], q_rs.at[4], to_up).wait_recv()
    rcopy(fin_m.at[hi], fin_m.at[hi], q_ss.at[5], q_rs.at[5], to_dn).wait_recv()
    qb[...] = (s_own[...] + fin_p[...] + fin_m[...]).astype(BF16).reshape(qb.shape)
    for k in range(1, nm):
        t = _mod(j + k, nm)
        go(rcopy(qb.at[t], qr.at[j], a_ss.at[k], a_rs.at[k], row(t)))
    qr[j] = qb[j]

    s_west, s_east, s_far = west * CORES + c, east * CORES + c, far * CORES + c
    rcopy(wo_rel.at[0], wo_rel.at[0], w_ss.at[2], w_rs.at[2], partner).wait_recv()
    go(rcopy(wo_rel.at[0], wo_v.at[s_west, wo_lo], w_ss.at[4], w_rs.at[4], dev(i, east, c)))
    rcopy(wo_rel.at[1], wo_rel.at[1], w_ss.at[3], w_rs.at[3], partner).wait_recv()
    go(rcopy(wo_rel.at[1], wo_v.at[s_east, wo_hi], w_ss.at[5], w_rs.at[5], dev(i, west, c)))
    ld_wo.wait()

    def to_core(n, ref):
        go(rcopy(ref, ref, d_ss.at[n], d_rs.at[n], partner))

    def wo_here(n, ref):
        rcopy(ref, ref, w_ss.at[n], w_rs.at[n], partner).wait_recv()
        return ref

    to_core(0, wo_v.at[j])
    to_core(1, wo_here(0, wo_v.at[s_west]))
    to_core(2, wo_here(1, wo_v.at[s_east]))

    kv32[0] = kn_ref[pl.ds(start, bl), :].astype(F32)
    kv32[1] = vn_ref[pl.ds(start, bl), :].astype(F32)
    ld_k.wait()
    ld_v.wait()

    for k in range(1, nm):
        src = _mod(j - k, nm)
        rcopy(qr.at[src], qr.at[src], a_ss.at[k], a_rs.at[k], partner).wait_recv()
    for jj in range(nm):
        for h in range(hl):
            for n in range(nl):
                q32[n, (jj * hl + h) * bl:(jj * hl + h + 1) * bl, :] = (
                    qr[jj, :, h * dh + n * LANES:h * dh + (n + 1) * LANES].astype(F32))

    def attend(b, _):
        q = jnp.concatenate([q32[n, pl.ds(b, H, stride=bl), :] for n in range(nl)], axis=1)
        s = lax.dot_general(q.astype(BF16), k_v[b], (((1,), (1,)), ((), ())), preferred_element_type=F32) * scale
        n = lens_ref[start + b]
        s = jnp.where(lax.broadcasted_iota(jnp.int32, (H, T), 1) < n, s, -jnp.inf)
        sn = jnp.sum(q * kv32[0, pl.ds(b, 1), :], axis=1, keepdims=True) * scale
        m = jnp.maximum(jnp.max(s, axis=1, keepdims=True), sn)
        p = jnp.exp(s - m)
        pn = jnp.exp(sn - m)
        l = jnp.sum(p, axis=1, keepdims=True) + pn
        acc = jnp.dot(p.astype(BF16), v_v[b], preferred_element_type=F32)
        acc = acc + pn.astype(BF16).astype(F32) * kv32[1, pl.ds(b, 1), :]
        o = acc / l
        for n in range(nl):
            o32[n, pl.ds(b, H, stride=bl), :] = o[:, n * LANES:(n + 1) * LANES]
        return 0

    lax.fori_loop(0, bl, attend, 0, unroll=8)

    wo_here(4, wo_v.at[s_far, wo_lo])
    wo_here(5, wo_v.at[s_far, wo_hi])
    to_core(3, wo_v.at[s_far])
    chip = i * nx + X
    for h in range(H):
        for n in range(nl):
            o_all[h, chip, :, n * LANES:(n + 1) * LANES] = o32[n, h * bl:(h + 1) * bl, :].astype(BF16)

    def gather(piece, ss, rs, arrived):
        class Half:
            def __init__(self, n):
                self.base, self.q = n * 20, 2 * n
                self.x_first = n == 0

            def piece(self, dp, ds, q, n):
                if self.x_first:
                    return piece(_mod(i + ds, ne), _mod(X + dp, nx), self.q + q, n)
                return piece(_mod(i + dp, ne), _mod(X + ds, nx), self.q + q, n)

            def to(self, dp, ds):
                if self.x_first:
                    return dev(_mod(i + ds, ne), _mod(X + dp, nx), c)
                return dev(_mod(i + dp, ne), _mod(X + ds, nx), c)

            def send(self, mid, ref, to):
                go(rcopy(ref, ref, ss.at[self.base + mid], rs.at[self.base + mid], to))

            def wait(self, mid, ref):
                rcopy(ref, ref, ss.at[self.base + mid], rs.at[self.base + mid], partner).wait_recv()
                arrived(ref)

            def s1(self):
                for d, sg in enumerate((1, -1)):
                    self.send(d, self.piece(0, 0, 0, 2), self.to(sg, 0))

            def w1s2(self):
                for d, sg in enumerate((1, -1)):
                    self.wait(d, self.piece(-sg, 0, 0, 2))
                    self.send(2 + d, self.piece(-sg, 0, d, 1), self.to(sg, 0))

            def w2(self):
                for d, sg in enumerate((1, -1)):
                    self.wait(2 + d, self.piece(2, 0, d, 1))

            def s3(self, k):
                for d, sg in enumerate((1, -1)):
                    self.send(4 + 2 * k + d, self.piece(ITEMS[k], 0, 0, 2), self.to(0, sg))

            def w3s4(self, k):
                for d, sg in enumerate((1, -1)):
                    self.wait(4 + 2 * k + d, self.piece(ITEMS[k], -sg, 0, 2))
                    self.send(12 + 2 * k + d, self.piece(ITEMS[k], -sg, d, 1), self.to(0, sg))

            def w4(self, k):
                for d, sg in enumerate((1, -1)):
                    self.wait(12 + 2 * k + d, self.piece(ITEMS[k], 2, d, 1))

        ITEMS = (0, -1, 1, 2)
        halves = (Half(0), Half(1))

        def both(name, *a):
            for hf in halves:
                getattr(hf, name)(*a)

        both('s1')
        both('s3', 0)
        arrived(piece(i, X, 0, 4))
        both('w1s2')
        both('s3', 1)
        both('s3', 2)
        both('w3s4', 0)
        both('w2')
        both('s3', 3)
        both('w3s4', 1)
        both('w3s4', 2)
        both('w3s4', 3)
        for k in range(4):
            both('w4', k)

    hq = H // 4
    gather(lambda yy, xx, q, n: o_all.at[pl.ds(q * hq, n * hq), yy * nx + xx], o_ss, o_rs, lambda ref: None)

    for k, src in enumerate((X, west, east, far)):
        ref = wo_v.at[src * CORES + 1 - c]
        rcopy(ref, ref, d_ss.at[k], d_rs.at[k], partner).wait_recv()

    rows = ne * nx * bl
    acc = None
    for h in range(H):
        t = jnp.dot(o_all[h].reshape(rows, dh), wo_v[h // hl, (h % hl) * dh:(h % hl + 1) * dh, :],
                    preferred_element_type=F32)
        acc = t if acc is None else acc + t
    cols = pl.ds(pl.multiple_of(chip * nw, nw), nw)
    mine = pl.ds(pl.multiple_of(X * nw, nw), nw)
    for r in range(ne):
        for xx in range(nx):
            g = (r * nx + xx) * bl
            res = xv[i, pl.ds(pl.multiple_of(r * be + (xx * CORES + c) * bl, bl), bl), mine].astype(F32)
            y_ref[r, xx, c, :, cols] = (res + acc[g:g + bl, :].astype(BF16).astype(F32)).astype(BF16)

    def to_partner(ref):
        rcopy(ref, ref, c_ss, c_rs, partner).start()

    gather(lambda yy, xx, q, n: y_ref.at[pl.ds(q, n), :, c, :, pl.ds(pl.multiple_of((yy * nx + xx) * nw, nw), nw)],
           y_ss, y_rs, to_partner)

    other, own = y_ref.at[:, :, 1 - c], y_ref.at[:, :, c]
    rcopy(own, other, c_ss, c_rs, partner).wait_recv()
    rcopy(own, other, c_ss, c_rs, partner).wait_send()
    for cp in sends:
        cp.wait_send()


def _write_out(y_in, kn_in, vn_in, y_out, kn_out, vn_out, sem):
    copies = [pltpu.make_async_copy(a, b, sem.at[n])
              for n, (a, b) in enumerate(((y_in, y_out), (kn_in, kn_out), (vn_in, vn_out)))]
    for cp in copies:
        cp.start()
    for cp in copies:
        cp.wait()


def solution(mesh):
    ne = mesh.shape['emb']
    nm = mesh.shape['model']

    def local(x, Wq, Wk, Wv, Wo, Kc, Vc, lengths):
        b, d = x.shape
        de = Wq.shape[0]
        dh = Wk.shape[1]
        hl = Wq.shape[1] // dh
        H = hl * nm
        nx = nm // CORES
        be = b // ne
        bl = be // nm
        T = Kc.shape[1]
        nw = Wo.shape[1] // nx
        hd = hl * dh
        V = pltpu.VMEM
        DMA = pltpu.SemaphoreType.DMA
        hbm = pl.BlockSpec(memory_space=pltpu.HBM)
        vmem = pl.BlockSpec(memory_space=pltpu.VMEM)
        outs = pl.pallas_call(
            functools.partial(_kernel, ne, nm, H),
            out_shape=(V((ne, nx, CORES, bl, d), BF16), V((b, dh), BF16), V((b, dh), BF16)),
            in_specs=[pl.BlockSpec(memory_space=pltpu.SMEM)] + [hbm] * 7,
            out_specs=(vmem, vmem, vmem),
            scratch_shapes=[
                V((ne, b, de), BF16), V((de, hd), BF16), V((d, 2 * dh), BF16),
                V((bl, T, dh), BF16), V((bl, T, dh), BF16), V((nm, hd, nw), BF16),
                V((be, hd), F32), V((be, hd), F32), V((be, hd), F32), V((be, hd), F32),
                V((be // 2, hd), F32), V((be // 2, hd), F32), V((be, hd), F32), V((be, hd), F32),
                V((2, hd // 2, nw), BF16), V((nm, bl, hd), BF16), V((nm, bl, hd), BF16), V((dh // LANES, H * bl, LANES), F32),
                V((2, bl, dh), F32), V((dh // LANES, H * bl, LANES), F32), V((H, ne * nx, bl, dh), BF16),
                DMA((10,)), DMA((6,)), DMA((6,)), DMA((nm,)), DMA((nm,)), DMA((6,)), DMA((6,)),
                DMA((nx,)), DMA((nx,)), DMA((40,)), DMA((40,)), DMA((40,)), DMA((40,)), DMA, DMA,
            ],
            compiler_params=pltpu.CompilerParams(collective_id=0, has_side_effects=True,
                                                 vmem_limit_bytes=58 * 1024 * 1024),
        )(lengths, x, Wq, Wk, Wv, Wo, Kc, Vc)
        n = len(outs)
        y, kn, vn = pl.pallas_call(
            _write_out,
            out_shape=tuple(jax.ShapeDtypeStruct(o.shape, o.dtype) for o in outs),
            in_specs=[vmem] * n, out_specs=(pl.BlockSpec(memory_space=pl.ANY),) * n, scratch_shapes=[DMA((n,))],
            compiler_params=pltpu.CompilerParams(vmem_limit_bytes=1024 * 1024),
        )(*outs)
        return y.reshape(b, d), kn, vn

    in_specs = (P('rep', None), P('emb', 'model'), P(), P(), P('model', 'emb'),
                P('rep', None, None), P('rep', None, None), P('rep'))
    out_specs = (P('rep', None), P('rep', None), P('rep', None))
    return jax.shard_map(local, mesh=mesh, in_specs=in_specs, out_specs=out_specs, check_vma=False)
```

```python
import functools

import jax
import jax.numpy as jnp
from jax import lax
from jax.experimental import pallas as pl
from jax.experimental.pallas import tpu as pltpu
from jax.sharding import PartitionSpec as P

CORES = 2
LANES = 128
GROUPS = 2
F32 = jnp.float32
BF16 = jnp.bfloat16


def _mod(a, n):
    return lax.rem(a + 2 * n, n)


def _kernel(ne, nm, H, lens_ref, x_hbm, wq_hbm, wk_hbm, wv_hbm, wo_hbm, kc_hbm, vc_hbm,
            y_ref, kn_ref, vn_ref,
            xv, wq_v, wkv, k_v, v_v, wo_v, s_opp, s_up, s_dn, s_own, rel_p, rel_m, fin_p, fin_m,
            wo_rel, qb, qr, q32, kv32, o32, o_all,
            lsem, q_ss, q_rs, a_ss, a_rs, w_ss, w_rs, d_ss, d_rs, g_ss, o_rs, y_rs, c_ss, c_rs):
    nx = nm // CORES
    i = lax.axis_index('emb')
    j = lax.axis_index('model')
    X = lax.div(j, CORES)
    c = lax.rem(j, CORES)
    de = xv.shape[2]
    be = s_opp.shape[0]
    bl = qr.shape[2]
    nl = q32.shape[0]
    dh = nl * LANES
    hl = H // nm
    hd, nw = wo_v.shape[1:]
    bg = be // GROUPS
    T = k_v.shape[2]
    scale = dh ** -0.5

    def first(g):
        return pl.multiple_of(i * be + g * bg + j * bl, bl)

    def dev(yy, xx, cc):
        return {'emb': yy, 'model': xx * CORES + cc}

    def row(jj):
        return {'emb': i, 'model': jj}

    def rcopy(src, dst, ss, rs, to):
        return pltpu.make_async_remote_copy(src_ref=src, dst_ref=dst, send_sem=ss, recv_sem=rs,
                                            device_id=to, device_id_type=pl.DeviceIdType.MESH)

    up, dn, opp = _mod(i + 1, ne), _mod(i - 1, ne), _mod(i + 2, ne)
    partner = dev(i, X, 1 - c)

    barrier = pltpu.get_barrier_semaphore()
    for k in range(1, nm):
        pl.semaphore_signal(barrier, inc=1, device_id=row(_mod(j + k, nm)), device_id_type=pl.DeviceIdType.MESH)
    for yy in (up, dn):
        pl.semaphore_signal(barrier, inc=1, device_id={'emb': yy, 'model': j}, device_id_type=pl.DeviceIdType.MESH)

    def load(n, src, dst):
        cp = pltpu.make_async_copy(src, dst, lsem.at[n])
        cp.start()
        return cp

    def xblock(n, blk):
        return load(n, x_hbm.at[:, pl.ds(pl.multiple_of(blk * de, de), de)], xv.at[blk])

    ld_x = [xblock(0, i)]
    ld_wq = load(4, wq_hbm, wq_v)
    ld_x += [xblock(k, _mod(i + k, ne)) for k in range(1, ne)]
    ld_wk = load(5, wk_hbm, wkv.at[:, pl.ds(0, dh)])
    ld_wv = load(6, wv_hbm, wkv.at[:, pl.ds(dh, dh)])
    ld_kv = [(load(8 + 2 * g, kc_hbm.at[pl.ds(first(g), bl)], k_v.at[g]),
              load(9 + 2 * g, vc_hbm.at[pl.ds(first(g), bl)], v_v.at[g])) for g in range(GROUPS)]
    ld_wo = load(7, wo_hbm.at[:, pl.ds(pl.multiple_of(X * nw, nw), nw)], wo_v.at[j])

    sends = []

    def go(cp):
        cp.start()
        sends.append(cp)

    ld_x[0].wait()
    ld_wq.wait()

    def part(d, buf):
        buf[...] = jnp.dot(xv[i, pl.ds(pl.multiple_of(d * be, be), be), :], wq_v[...], preferred_element_type=F32)

    hb = bg // 2
    to_up, to_dn = {'emb': up, 'model': j}, {'emb': dn, 'model': j}

    def lo(g):
        return pl.ds(g * bg, hb)

    def hi(g):
        return pl.ds(g * bg + hb, hb)

    def q_copy(n, g, src, dst, to):
        return rcopy(src, dst, q_ss.at[6 * g + n], q_rs.at[6 * g + n], to)

    def send_opp(g):
        go(q_copy(0, g, s_opp.at[lo(g)], rel_p.at[g], to_up))
        go(q_copy(1, g, s_opp.at[hi(g)], rel_m.at[g], to_dn))

    def send_pure_up(g):
        go(q_copy(2, g, s_up.at[hi(g)], fin_p.at[hi(g)], to_up))

    def send_pure_dn(g):
        go(q_copy(3, g, s_dn.at[lo(g)], fin_m.at[lo(g)], to_dn))

    def relay(g):
        q_copy(0, g, rel_p.at[g], rel_p.at[g], to_up).wait_recv()
        s_up[lo(g), :] = s_up[lo(g), :] + rel_p[g]
        go(q_copy(4, g, s_up.at[lo(g)], fin_p.at[lo(g)], to_up))
        q_copy(1, g, rel_m.at[g], rel_m.at[g], to_dn).wait_recv()
        s_dn[hi(g), :] = s_dn[hi(g), :] + rel_m[g]
        go(q_copy(5, g, s_dn.at[hi(g)], fin_m.at[hi(g)], to_dn))

    def exchange(g):
        for n, ref, to in ((2, fin_p.at[hi(g)], to_up), (3, fin_m.at[lo(g)], to_dn),
                           (4, fin_p.at[lo(g)], to_up), (5, fin_m.at[hi(g)], to_dn)):
            q_copy(n, g, ref, ref, to).wait_recv()
        rows = slice(g * bg, (g + 1) * bg)
        qb[g] = (s_own[rows, :] + fin_p[rows, :] + fin_m[rows, :]).reshape(qb.shape[1:]).astype(BF16)
        for k in range(1, nm):
            t = _mod(j + k, nm)
            go(rcopy(qb.at[g, t], qr.at[g, j], a_ss.at[g * nm + k], a_rs.at[g * nm + k], row(t)))
        qr[g, j] = qb[g, j]

    part(opp, s_opp)
    pl.semaphore_wait(barrier, nm - 1 + 2)
    send_opp(0)
    part(up, s_up)
    send_pure_up(0)
    part(dn, s_dn)
    send_pure_dn(0)
    send_opp(1)

    east, west, far = _mod(X + 1, nx), _mod(X - 1, nx), _mod(X + 2, nx)
    wo_lo, wo_hi = pl.ds(0, hd // 2), pl.ds(hd // 2, hd // 2)

    def wo_cols(rows, t):
        return wo_hbm.at[rows, pl.ds(pl.multiple_of(t * nw, nw), nw)]

    go(rcopy(wo_cols(pl.ds(0, hd), east), wo_v.at[j], w_ss.at[0], w_rs.at[0], dev(i, east, c)))
    go(rcopy(wo_cols(pl.ds(0, hd), west), wo_v.at[j], w_ss.at[1], w_rs.at[1], dev(i, west, c)))
    go(rcopy(wo_cols(wo_lo, far), wo_rel.at[0], w_ss.at[2], w_rs.at[2], dev(i, east, c)))
    go(rcopy(wo_cols(wo_hi, far), wo_rel.at[1], w_ss.at[3], w_rs.at[3], dev(i, west, c)))
    part(i, s_own)

    for ld in ld_x[1:]:
        ld.wait()
    ld_wk.wait()
    ld_wv.wait()

    rows_m = kn_ref.shape[0] // ne

    def kv_rows(m, _):
        rows = pl.ds(pl.multiple_of(m * rows_m, rows_m), rows_m)
        acc = jnp.dot(xv[0, rows, :], wkv[0:de, :], preferred_element_type=F32)
        for blk in range(1, ne):
            acc = acc + jnp.dot(xv[blk, rows, :], wkv[blk * de:(blk + 1) * de, :], preferred_element_type=F32)
        acc = acc.astype(BF16)
        kn_ref[rows, :] = acc[:, :dh]
        vn_ref[rows, :] = acc[:, dh:]
        kv32[rows, :] = acc.astype(F32)
        return 0

    lax.fori_loop(0, ne, kv_rows, 0)

    relay(0)
    send_pure_up(1)
    send_pure_dn(1)
    relay(1)
    exchange(0)
    exchange(1)

    s_west, s_east, s_far = west * CORES + c, east * CORES + c, far * CORES + c
    rcopy(wo_rel.at[0], wo_rel.at[0], w_ss.at[2], w_rs.at[2], partner).wait_recv()
    go(rcopy(wo_rel.at[0], wo_v.at[s_west, wo_lo], w_ss.at[4], w_rs.at[4], dev(i, east, c)))
    rcopy(wo_rel.at[1], wo_rel.at[1], w_ss.at[3], w_rs.at[3], partner).wait_recv()
    go(rcopy(wo_rel.at[1], wo_v.at[s_east, wo_hi], w_ss.at[5], w_rs.at[5], dev(i, west, c)))
    ld_wo.wait()

    def to_core(n, ref):
        go(rcopy(ref, ref, d_ss.at[n], d_rs.at[n], partner))

    def wo_here(n, ref):
        rcopy(ref, ref, w_ss.at[n], w_rs.at[n], partner).wait_recv()
        return ref

    to_core(0, wo_v.at[j])
    to_core(1, wo_here(0, wo_v.at[s_west]))
    to_core(2, wo_here(1, wo_v.at[s_east]))

    chip = i * nx + X

    def attention(g):
        for ld in ld_kv[g]:
            ld.wait()
        for k in range(1, nm):
            src = qr.at[g, _mod(j - k, nm)]
            rcopy(src, src, a_ss.at[g * nm + k], a_rs.at[g * nm + k], partner).wait_recv()
        for jj in range(nm):
            for h in range(hl):
                for n in range(nl):
                    q32[n, (jj * hl + h) * bl:(jj * hl + h + 1) * bl, :] = (
                        qr[g, jj, :, h * dh + n * LANES:h * dh + (n + 1) * LANES].astype(F32))
        new = kv32[pl.ds(first(g), bl), :]
        for b in range(bl):
            q = jnp.concatenate([q32[n, pl.ds(b, H, stride=bl), :] for n in range(nl)], axis=1)
            s = lax.dot_general(q.astype(BF16), k_v[g, b], (((1,), (1,)), ((), ())),
                                preferred_element_type=F32) * scale
            s = jnp.where(lax.broadcasted_iota(jnp.int32, (H, T), 1) < lens_ref[first(g) + b], s, -jnp.inf)
            sn = jnp.sum(q * new[b:b + 1, :dh], axis=1, keepdims=True) * scale
            m = jnp.maximum(jnp.max(s, axis=1, keepdims=True), sn)
            p = jnp.exp(s - m)
            pn = jnp.exp(sn - m)
            l = jnp.sum(p, axis=1, keepdims=True) + pn
            acc = jnp.dot(p.astype(BF16), v_v[g, b], preferred_element_type=F32)
            acc = acc + pn.astype(BF16).astype(F32) * new[b:b + 1, dh:]
            o = acc / l
            for n in range(nl):
                o32[n, pl.ds(b, H, stride=bl), :] = o[:, n * LANES:(n + 1) * LANES]
        for h in range(H):
            for n in range(nl):
                o_all[g, h, chip, :, n * LANES:(n + 1) * LANES] = o32[n, h * bl:(h + 1) * bl, :].astype(BF16)

    class Gather:
        ITEMS = (0, -1, 1, 2)

        def __init__(self, piece, ss, rs, base, arrived):
            self.p, self.ss, self.rs, self.base, self.arrived = piece, ss, rs, base, arrived

        def piece(self, hf, dp, ds, q, n):
            dx, dy = (dp, ds) if hf == 0 else (ds, dp)
            return self.p(_mod(i + dy, ne), _mod(X + dx, nx), 2 * hf + q, n)

        def to(self, hf, dp, ds):
            dx, dy = (dp, ds) if hf == 0 else (ds, dp)
            return dev(_mod(i + dy, ne), _mod(X + dx, nx), c)

        def send(self, hf, mid, ref, to):
            rcopy(ref, ref, self.ss, self.rs.at[self.base + 20 * hf + mid], to).start()

        def wait(self, hf, mid, ref):
            rcopy(ref, ref, self.ss, self.rs.at[self.base + 20 * hf + mid], partner).wait_recv()
            self.arrived(ref)

        def near(self, k):
            for hf in range(2):
                for d, sg in enumerate((1, -1)):
                    self.send(hf, 4 + 2 * k + d, self.piece(hf, self.ITEMS[k], 0, 0, 2), self.to(hf, 0, sg))

        def start(self):
            for hf in range(2):
                for d, sg in enumerate((1, -1)):
                    self.send(hf, d, self.piece(hf, 0, 0, 0, 2), self.to(hf, sg, 0))
            self.near(0)
            self.arrived(self.p(i, X, 0, 4))

        def first(self):
            for hf in range(2):
                for d, sg in enumerate((1, -1)):
                    self.wait(hf, d, self.piece(hf, -sg, 0, 0, 2))
                    self.send(hf, 2 + d, self.piece(hf, -sg, 0, d, 1), self.to(hf, sg, 0))
            self.near(1)
            self.near(2)

        def second(self):
            for hf in range(2):
                for d, sg in enumerate((1, -1)):
                    self.wait(hf, 2 + d, self.piece(hf, 2, 0, d, 1))
            self.near(3)

        def on(self, k):
            for hf in range(2):
                for d, sg in enumerate((1, -1)):
                    self.wait(hf, 4 + 2 * k + d, self.piece(hf, self.ITEMS[k], -sg, 0, 2))
                    self.send(hf, 12 + 2 * k + d, self.piece(hf, self.ITEMS[k], -sg, d, 1), self.to(hf, 0, sg))

        def end(self):
            for k in range(4):
                for hf in range(2):
                    for d, sg in enumerate((1, -1)):
                        self.wait(hf, 12 + 2 * k + d, self.piece(hf, self.ITEMS[k], 2, d, 1))

    hq = H // 4

    def o_gather(g):
        return Gather(lambda yy, xx, q, n: o_all.at[g, pl.ds(q * hq, n * hq), yy * nx + xx],
                      g_ss.at[g], o_rs, 40 * g, lambda ref: None)

    def to_partner(ref):
        rcopy(ref, ref, c_ss, c_rs, partner).start()

    def y_gather(g):
        return Gather(lambda yy, xx, q, n: y_ref.at[pl.ds(q, n), g, :, c, :,
                                                    pl.ds(pl.multiple_of((yy * nx + xx) * nw, nw), nw)],
                      g_ss.at[GROUPS + g], y_rs, 40 * g, to_partner)

    cols = pl.ds(pl.multiple_of(chip * nw, nw), nw)
    mine = pl.ds(pl.multiple_of(X * nw, nw), nw)

    def product(g):
        rows = ne * nx * bl
        acc = None
        for h in range(H):
            t = jnp.dot(o_all[g, h].astype(F32).reshape(rows, dh).astype(BF16),
                        wo_v[h // hl, (h % hl) * dh:(h % hl + 1) * dh, :], preferred_element_type=F32)
            acc = t if acc is None else acc + t
        for r in range(ne):
            for xx in range(nx):
                n = (r * nx + xx) * bl
                res = xv[i, pl.ds(r * be + g * bg + xx * CORES * bl, CORES * bl), mine].astype(F32)
                res = jnp.where(c == 0, res[:bl], res[bl:])
                y_ref[r, g, xx, c, :, cols] = (res + acc[n:n + bl, :].astype(BF16).astype(F32)).astype(BF16)

    o0, o1, y0, y1 = o_gather(0), o_gather(1), y_gather(0), y_gather(1)
    attention(0)
    o0.start()
    attention(1)
    o1.start()
    wo_here(4, wo_v.at[s_far, wo_lo])
    wo_here(5, wo_v.at[s_far, wo_hi])
    to_core(3, wo_v.at[s_far])
    o0.first()
    o0.on(0)
    o0.second()
    o1.first()
    o0.on(1)
    o0.on(2)
    o1.on(0)
    o1.second()
    o0.on(3)
    o1.on(1)
    o1.on(2)
    o0.end()

    for k, src in enumerate((X, west, east, far)):
        ref = wo_v.at[src * CORES + 1 - c]
        rcopy(ref, ref, d_ss.at[k], d_rs.at[k], partner).wait_recv()
    product(0)
    y0.start()
    o1.on(3)
    o1.end()
    product(1)
    y1.start()
    y0.first()
    y0.on(0)
    y0.second()
    y1.first()
    y0.on(1)
    y0.on(2)
    y1.on(0)
    y1.second()
    y0.on(3)
    y1.on(1)
    y1.on(2)
    y0.end()
    y1.on(3)
    y1.end()

    other, own = y_ref.at[:, :, :, 1 - c], y_ref.at[:, :, :, c]
    rcopy(own, other, c_ss, c_rs, partner).wait_recv()
    rcopy(own, other, c_ss, c_rs, partner).wait_send()
    chips = ne * nx - 1
    for g in range(GROUPS):
        ref = o_all.at[g, :, pl.ds(0, chips)]
        rcopy(ref, ref, g_ss.at[g], o_rs.at[0], partner).wait_send()
        ref = y_ref.at[:, g, :, c, :, pl.ds(0, chips * nw)]
        rcopy(ref, ref, g_ss.at[GROUPS + g], y_rs.at[0], partner).wait_send()
    for cp in sends:
        cp.wait_send()


def _write_out(y_in, kn_in, vn_in, y_out, kn_out, vn_out, sem):
    copies = [pltpu.make_async_copy(a, b, sem.at[n])
              for n, (a, b) in enumerate(((y_in, y_out), (kn_in, kn_out), (vn_in, vn_out)))]
    for cp in copies:
        cp.start()
    for cp in copies:
        cp.wait()


def solution(mesh):
    ne = mesh.shape['emb']
    nm = mesh.shape['model']

    def local(x, Wq, Wk, Wv, Wo, Kc, Vc, lengths):
        b, d = x.shape
        de = Wq.shape[0]
        dh = Wk.shape[1]
        hl = Wq.shape[1] // dh
        H = hl * nm
        nx = nm // CORES
        be = b // ne
        bl = be // (nm * GROUPS)
        T = Kc.shape[1]
        nw = Wo.shape[1] // nx
        hd = hl * dh
        V = pltpu.VMEM
        DMA = pltpu.SemaphoreType.DMA
        hbm = pl.BlockSpec(memory_space=pltpu.HBM)
        vmem = pl.BlockSpec(memory_space=pltpu.VMEM)
        outs = pl.pallas_call(
            functools.partial(_kernel, ne, nm, H),
            out_shape=(V((ne, GROUPS, nx, CORES, bl, d), BF16), V((b, dh), BF16), V((b, dh), BF16)),
            in_specs=[pl.BlockSpec(memory_space=pltpu.SMEM)] + [hbm] * 7,
            out_specs=(vmem, vmem, vmem),
            scratch_shapes=[
                V((ne, b, de), BF16), V((de, hd), BF16), V((d, 2 * dh), BF16),
                V((GROUPS, bl, T, dh), BF16), V((GROUPS, bl, T, dh), BF16), V((nm, hd, nw), BF16),
                V((be, hd), F32), V((be, hd), F32), V((be, hd), F32), V((be, hd), F32),
                V((GROUPS, be // GROUPS // 2, hd), F32), V((GROUPS, be // GROUPS // 2, hd), F32),
                V((be, hd), F32), V((be, hd), F32),
                V((2, hd // 2, nw), BF16), V((GROUPS, nm, bl, hd), BF16), V((GROUPS, nm, bl, hd), BF16),
                V((dh // LANES, H * bl, LANES), F32), V((b, 2 * dh), F32),
                V((dh // LANES, H * bl, LANES), F32), V((GROUPS, H, ne * nx, bl, dh), BF16),
                DMA((8 + 2 * GROUPS,)), DMA((6 * GROUPS,)), DMA((6 * GROUPS,)),
                DMA((nm * GROUPS,)), DMA((nm * GROUPS,)), DMA((6,)), DMA((6,)),
                DMA((nx,)), DMA((nx,)), DMA((2 * GROUPS,)), DMA((40 * GROUPS,)), DMA((40 * GROUPS,)), DMA, DMA,
            ],
            compiler_params=pltpu.CompilerParams(collective_id=0, has_side_effects=True,
                                                 vmem_limit_bytes=58 * 1024 * 1024),
        )(lengths, x, Wq, Wk, Wv, Wo, Kc, Vc)
        n = len(outs)
        y, kn, vn = pl.pallas_call(
            _write_out,
            out_shape=tuple(jax.ShapeDtypeStruct(o.shape, o.dtype) for o in outs),
            in_specs=[vmem] * n, out_specs=(pl.BlockSpec(memory_space=pl.ANY),) * n, scratch_shapes=[DMA((n,))],
            compiler_params=pltpu.CompilerParams(vmem_limit_bytes=1024 * 1024),
        )(*outs)
        return y.reshape(b, d), kn, vn

    in_specs = (P('rep', None), P('emb', 'model'), P(), P(), P('model', 'emb'),
                P('rep', None, None), P('rep', None, None), P('rep'))
    out_specs = (P('rep', None), P('rep', None), P('rep', None))
    return jax.shard_map(local, mesh=mesh, in_specs=in_specs, out_specs=out_specs, check_vma=False)
```
